32 devices in a mesh: gz: 2 (over core), dp: 16 (over z, y, x).
Axes of the slice: x: 2, y: 2, z: 4, core: 2. Of those that a mesh axis runs over, the one named last changes fastest.
Arguments:
- inputs: bfloat16 [16, 32, 16, 8, 128], P('dp', None, 'gz'), may hold values from -6 to 6
- kernel_one: bfloat16 [32, 32, 3, 3, 3], replicated, may hold values from -0.21875 to 0.21875
- kernel_two: bfloat16 [32, 32, 3, 3, 3], replicated, may hold values from -0.21875 to 0.21875
- cotangent: bfloat16 [16, 32, 16, 8, 128], P('dp', None, 'gz'), may hold values from -12 to 12
Outputs:
- input_grad: bfloat16 [16, 32, 16, 8, 128], P('dp', None, 'gz')
- kernel_one_grad: float32 [32, 32, 3, 3, 3], replicated
- kernel_two_grad: float32 [32, 32, 3, 3, 3], replicated
The draws below stay inside these ranges and needn't reach their ends.
All inputs are finite; a program needn't handle non-finite values.
Results may differ from the reference program's by a relative error of at most 0.006.
Values may be sent and summed in bfloat16 or wider, within the bound.
A program may use at most 64 MiB of HBM per device.

```python
import math
import jax
import jax.numpy as jnp
from jax import lax

C = 32
NY = 8
NX = 128
NZ = 16
BATCH = 16


def draw_cotangent(key, part):
    sample_pos = jnp.arange(BATCH, dtype=jnp.float32) / max(BATCH - 1, 1)
    plane_pos = jnp.arange(NZ, dtype=jnp.float32) / max(NZ - 1, 1)
    scale = 1.0 + sample_pos[:, None, None, None, None] + plane_pos[None, None, :, None, None]
    base = jnp.clip(jax.random.normal(key, (BATCH, C, NZ, NY, NX), jnp.float32), -4.0, 4.0)
    return (base * scale).astype(jnp.bfloat16)


def steps_of(stream_key, extent, split, low, high):
    def one(position, parts):
        draws = jax.random.uniform(jax.random.fold_in(jax.random.fold_in(stream_key, 6), position), (parts,), jnp.float32, low / len(split), high / len(split))
        return jnp.repeat(jnp.exp(draws), extent[position] // parts).reshape((-1,) + (1,) * (len(extent) - position - 1))

    gain = one(*split[0])
    for cut in split[1:]:
        gain = gain * one(*cut)
    return gain


def normal_values(rng, extent, spread, most, pieces=(), held_as=jnp.bfloat16):
    entries = spread * jax.random.normal(rng, extent, jnp.float32)
    if pieces:
        entries = entries * steps_of(rng, extent, pieces, -0.22, 0.18)
    return jnp.clip(entries, -most, most).astype(held_as)


def setup_inputs(seed: int = 0) -> dict:
    streams_of = jax.random.split(jax.random.key(seed), 5)
    return {
        "inputs": normal_values(streams_of[0], (BATCH, C, NZ, NY, NX), 1.0, 6.0, ((0, 16), (2, 2))),
        "kernel_one": normal_values(streams_of[1], (C, C, 3, 3, 3), (27 * C) ** -0.5, 0.21875),
        "kernel_two": normal_values(streams_of[2], (C, C, 3, 3, 3), (27 * C) ** -0.5, 0.21875),
        "cotangent": draw_cotangent(jax.random.fold_in(streams_of[4], 71), 0),
    }


def convolve(field, kernel):
    out = lax.conv_general_dilated(field[None], kernel, (1, 1, 1), ((1, 1), (1, 1), (1, 1)), dimension_numbers=('NCDHW', 'OIDHW', 'NCDHW'), preferred_element_type=jnp.float32)
    return out[0]

def flipped(kernel):
    return jnp.swapaxes(jnp.flip(kernel, (2, 3, 4)), 0, 1)

def kernel_terms(padded, grad):
    out = lax.conv_general_dilated(padded[None], grad[None], (1, 1, 1), 'VALID', dimension_numbers=('CNDHW', 'IODHW', 'NCDHW'), preferred_element_type=jnp.float32)
    return jnp.transpose(out, (1, 0, 2, 3, 4))

def dsilu(value):
    sig = jax.nn.sigmoid(value)
    return sig * (1.0 + value * (1.0 - sig))

def one_sample(pair, kernel_one, kernel_two):
    source, upstream = pair
    pre_one = convolve(source, kernel_one)
    hidden = jax.nn.silu(pre_one).astype(jnp.bfloat16)
    pre_two = convolve(hidden, kernel_two)
    grad_two = (upstream.astype(jnp.float32) * dsilu(pre_two)).astype(jnp.bfloat16)
    hidden_grad = convolve(grad_two, flipped(kernel_two))
    grad_one = (hidden_grad * dsilu(pre_one)).astype(jnp.bfloat16)
    input_grad = convolve(grad_one, flipped(kernel_one)).astype(jnp.bfloat16)
    widths = ((0, 0), (1, 1), (1, 1), (1, 1))
    term_two = kernel_terms(jnp.pad(hidden, widths), grad_two)
    term_one = kernel_terms(jnp.pad(source, widths), grad_one)
    return (input_grad, term_one, term_two)

def reference(inputs, kernel_one, kernel_two, cotangent):
    input_grad, terms_one, terms_two = lax.map(lambda pair: one_sample(pair, kernel_one, kernel_two), (inputs, cotangent))
    factor = 1.0 / math.sqrt(BATCH * NZ * NY * NX)
    return (input_grad, lax.optimization_barrier(jnp.sum(terms_one, axis=0)) * factor, lax.optimization_barrier(jnp.sum(terms_two, axis=0)) * factor)
```

```python
import functools
import math

import jax
import jax.numpy as jnp
from jax import lax
from jax.experimental import pallas as pl
from jax.experimental.pallas import tpu as pltpu
from jax.sharding import PartitionSpec as P

MESH = pl.DeviceIdType.MESH
F32 = jnp.float32
BF16 = jnp.bfloat16
TAPS = [(plane, col) for plane in range(3) for col in range(3)]
NN = (((1,), (0,)), ((), ()))
NT = (((1,), (1,)), ((), ()))


def dot(a, b, dims=NN):
    return lax.dot_general(a, b, dims, preferred_element_type=F32)


def iota(shape, dim):
    return lax.broadcasted_iota(jnp.int32, shape, dim)


def one_hot(mask):
    return jnp.where(mask, 1.0, 0.0).astype(BF16)


def sigmoid(v):
    return 0.5 * jnp.tanh(0.5 * v) + 0.5


def kernel(
    sizes,
    factor,
    x_ref,
    w1_ref,
    w2_ref,
    cot_ref,
    out_ref,
    g1_ref,
    g2_ref,
    s_in,
    s_hid,
    s_g2,
    s_g1,
    wcat,
    slope,
    bands,
    packed,
    arrived,
    full,
    halo_send,
    halo_recv,
    rs_send,
    rs_recv,
    ag_send,
    ag_recv,
):
    gz_count, dp_count, owners = sizes
    chan, depth, height, width = x_ref.shape
    rows = chan * height
    count = gz_count * dp_count
    gz = lax.axis_index("gz")
    dp = lax.axis_index("dp")
    me = gz * dp_count + dp

    def place(dev):
        return {"gz": dev // dp_count, "dp": lax.rem(dev, dp_count)}

    barrier = pltpu.get_barrier_semaphore()

    def greet(k, carry):
        dev = lax.rem(me + k, count)
        pl.semaphore_signal(barrier, inc=1, device_id=place(dev), device_id_type=MESH)
        return carry

    lax.fori_loop(1, count, greet, 0)

    r, l = iota((rows, rows), 0), iota((rows, rows), 1)
    to_rows = one_hot((r // chan == l % height) & (r % chan == l // height))
    to_chan = one_hot((r // height == l % chan) & (r % height == l // chan))

    def shifts(s, p, value):
        lane = iota(value.shape, 1)
        s[0, p] = jnp.where(lane == 0, 0.0, pltpu.roll(value, 1, 1)).astype(BF16)
        s[2, p] = jnp.where(lane == width - 1, 0.0, pltpu.roll(value, width - 1, 1)).astype(BF16)

    def put(s, p, value):
        s[1, p] = value.astype(BF16)
        shifts(s, p, value)

    def up_copy(n, s):
        return pltpu.make_async_remote_copy(
            src_ref=s.at[1, depth],
            dst_ref=s.at[1, 0],
            send_sem=halo_send.at[n, 0],
            recv_sem=halo_recv.at[n, 0],
            device_id={"gz": gz + 1, "dp": dp},
            device_id_type=MESH,
        )

    def down_copy(n, s):
        return pltpu.make_async_remote_copy(
            src_ref=s.at[1, 1],
            dst_ref=s.at[1, depth + 1],
            send_sem=halo_send.at[n, 1],
            recv_sem=halo_recv.at[n, 1],
            device_id={"gz": gz - 1, "dp": dp},
            device_id_type=MESH,
        )

    def send_halo(n, s):
        @pl.when(gz < gz_count - 1)
        def _():
            up_copy(n, s).start()

        @pl.when(gz > 0)
        def _():
            down_copy(n, s).start()

    def take_halo(n, s):
        @pl.when(gz > 0)
        def _():
            up_copy(n, s).wait_recv()

        @pl.when(gz == 0)
        def _():
            s[1, 0] = jnp.zeros((rows, width), BF16)

        @pl.when(gz < gz_count - 1)
        def _():
            down_copy(n, s).wait_recv()

        @pl.when(gz == gz_count - 1)
        def _():
            s[1, depth + 1] = jnp.zeros((rows, width), BF16)

        for p in (0, depth + 1):
            shifts(s, p, s[1, p].astype(F32))

    def raw(ref, p):
        return ref[:, p].astype(F32).reshape(rows, width).astype(BF16)

    edges = sorted({0, depth - 1})
    inner = [p for p in range(depth) if p not in edges]
    groups = [edges] + [inner[i : i + 2] for i in range(0, len(inner), 2)]

    def lanes(parts):
        return parts[0] if len(parts) == 1 else jnp.concatenate(parts, axis=1)

    def load(ref, planes):
        value = dot(to_rows, lanes([raw(ref, p) for p in planes]))
        return [value[:, i * width : (i + 1) * width] for i in range(len(planes))]

    def conv(n, s, planes):
        window = jnp.concatenate(
            [lanes([s[col, p + plane] for p in planes]) for plane, col in TAPS], axis=0
        )
        value = dot(wcat[n], window)
        return [value[:, i * width : (i + 1) * width] for i in range(len(planes))]

    for planes in groups:
        for p, value in zip(planes, load(x_ref, planes)):
            put(s_in, p + 1, value)

    pack = 4 * chan
    er, el = iota((chan, pack), 0), iota((chan, pack), 1)
    spots = [one_hot(el == er + off * chan) for off in range(3)]
    eye = one_hot(iota((chan, chan), 0) == iota((chan, chan), 1))
    pieces = []
    for ref in (w1_ref, w2_ref):
        base = None
        for off in range(3):
            tall = jnp.concatenate([ref[9 * a + 3 * off + b] for a, b in TAPS], axis=0)
            piece = dot(tall, spots[off])
            base = piece if base is None else base + piece
        pieces.append(base.astype(BF16))
    blank = jnp.zeros((chan, chan), BF16)
    for ref in (w2_ref, w1_ref):
        for a, b in TAPS:
            tall = jnp.concatenate(
                [ref[26 - (9 * a + 3 * off + b)] for off in range(3)] + [blank], axis=0
            )
            pieces.append(dot(eye, tall, NT).astype(BF16))
    base = jnp.concatenate(pieces, axis=0)
    sr, sl = iota((pack, rows), 0), iota((pack, rows), 1)
    for y in range(height):
        pick = one_hot(
            (sr % chan == sl % chan)
            & (sl // chan == y - 1 + sr // chan)
            & (sr < 3 * chan)
        )
        placed = dot(base, pick).astype(BF16)
        for n in range(4):
            for t in range(9):
                at = (n * 9 + t) * chan
                wcat[n, y * chan : (y + 1) * chan, t * rows : (t + 1) * rows] = placed[
                    at : at + chan
                ]

    pl.semaphore_wait(barrier, count - 1)
    send_halo(0, s_in)

    def scatter_terms(j):
        def step(k, carry):
            dev = lax.rem(me + k, count)

            @pl.when(dev < owners)
            def _():
                pltpu.make_async_remote_copy(
                    src_ref=packed.at[j, dev],
                    dst_ref=arrived.at[j, count - 1 - k],
                    send_sem=rs_send.at[j],
                    recv_sem=rs_recv.at[j],
                    device_id=place(dev),
                    device_id_type=MESH,
                ).start()

            return carry

        lax.fori_loop(1, count, step, 0)

    def wait_for(ref, sem):
        pltpu.make_async_copy(ref, ref, sem).wait()

    def gather_terms(j):
        @pl.when(me < owners)
        def _():
            wait_for(arrived.at[j], rs_recv.at[j])
            full[j, me] = (jnp.sum(arrived[j], axis=0) + packed[j, me]) * factor

            def step(k, carry):
                dev = lax.rem(me + k, count)
                pltpu.make_async_remote_copy(
                    src_ref=full.at[j, me],
                    dst_ref=full.at[j, me],
                    send_sem=ag_send.at[j],
                    recv_sem=ag_recv.at[j],
                    device_id=place(dev),
                    device_id_type=MESH,
                ).start()
                return carry

            lax.fori_loop(1, count, step, 0)

    def finish_terms(j, ref):
        @pl.when(me < owners)
        def _():
            wait_for(full.at[j, pl.ds(0, owners - 1)], ag_recv.at[j])
            wait_for(packed.at[j, pl.ds(0, owners - 1)], rs_send.at[j])
            wait_for(arrived.at[j], ag_send.at[j])

        @pl.when(me >= owners)
        def _():
            wait_for(full.at[j, pl.ds(0, owners)], ag_recv.at[j])
            wait_for(packed.at[j, pl.ds(0, owners)], rs_send.at[j])

        tiles = full.shape[2]
        value = full[j].reshape(owners * tiles, 8, 128)
        for g in range(4):
            ref[:, g * 8 : (g + 1) * 8, :] = value[:27, :, g * chan : (g + 1) * chan]

    qr, ql = iota((4 * rows, 128), 0), iota((4 * rows, 128), 1)
    gather_rows = one_hot((qr // rows == ql // chan) & (qr % chan == ql % chan))

    def terms(j, s, s_grad):
        grad = lanes([s_grad[1, p + 1] for p in range(depth)])
        block = iota((chan, rows), 1) // chan
        for plane, col in TAPS:
            window = lanes([s[col, p + plane] for p in range(depth)])
            value = dot(grad, window, NT)
            for off in range(3):
                band = jnp.zeros((chan, rows), F32)
                for y in range(height):
                    if 0 <= y + off - 1 < height:
                        part = value[y * chan : (y + 1) * chan]
                        band = jnp.where(block == y + off - 1, part, band)
                t = plane * 9 + off * 3 + col
                for g in range(4):
                    bands[t * 8 : (t + 1) * 8, g * rows : (g + 1) * rows] = band[
                        g * 8 : (g + 1) * 8
                    ]
        value = bands[...]
        high = value.astype(BF16)
        low = (value - high.astype(F32)).astype(BF16)
        total = (dot(high, gather_rows) + dot(low, gather_rows)).reshape(27, 8, 128)
        tiles = packed.shape[2]
        for t in range(27):
            packed[j, t // tiles, t % tiles] = total[t]

    if owners * packed.shape[2] > 27:
        packed[...] = jnp.zeros_like(packed)

    take_halo(0, s_in)
    for i, planes in enumerate(groups):
        for p, pre in zip(planes, conv(0, s_in, planes)):
            sig = sigmoid(pre)
            slope[p] = sig * (1.0 + pre * (1.0 - sig))
            put(s_hid, p + 1, pre * sig)
        if i == 0:
            send_halo(1, s_hid)
    take_halo(1, s_hid)
    for i, planes in enumerate(groups):
        for p, pre, cot in zip(planes, conv(1, s_hid, planes), load(cot_ref, planes)):
            sig = sigmoid(pre)
            put(s_g2, p + 1, cot * (sig * (1.0 + pre * (1.0 - sig))))
        if i == 0:
            send_halo(2, s_g2)
    terms(1, s_hid, s_g2)
    scatter_terms(1)
    take_halo(2, s_g2)
    for i, planes in enumerate(groups):
        for p, value in zip(planes, conv(2, s_g2, planes)):
            put(s_g1, p + 1, value * slope[p])
        if i == 0:
            send_halo(3, s_g1)
    gather_terms(1)
    terms(0, s_in, s_g1)
    scatter_terms(0)
    take_halo(3, s_g1)
    for planes in groups:
        value = lanes([v.astype(BF16) for v in conv(3, s_g1, planes)])
        value = dot(to_chan, value)
        for i, p in enumerate(planes):
            part = value[:, i * width : (i + 1) * width]
            out_ref[:, p] = part.reshape(chan, height, width).astype(BF16)
    gather_terms(0)
    finish_terms(1, g2_ref)
    finish_terms(0, g1_ref)

    for n, s in enumerate((s_in, s_hid, s_g2, s_g1)):

        @pl.when(gz < gz_count - 1)
        def _():
            up_copy(n, s).wait_send()

        @pl.when(gz > 0)
        def _():
            down_copy(n, s).wait_send()


def solution(mesh):
    gz_count, dp_count = mesh.shape["gz"], mesh.shape["dp"]
    count = gz_count * dp_count

    def local(inputs, kernel_one, kernel_two, cotangent):
        _, chan, depth, height, width = inputs.shape
        rows = chan * height
        cells = dp_count * gz_count * depth * height * width
        tiles = -(-27 // count)
        owners = -(-27 // tiles)
        taps = lambda k: k.transpose(2, 3, 4, 0, 1).reshape(27, chan, chan)
        slab = pltpu.VMEM((3, depth + 2, rows, width), BF16)
        vmem = pl.BlockSpec(memory_space=pltpu.VMEM)
        out, g1, g2 = pl.pallas_call(
            functools.partial(kernel, (gz_count, dp_count, owners), 1.0 / math.sqrt(cells)),
            out_shape=(
                jax.ShapeDtypeStruct((chan, depth, height, width), BF16),
                jax.ShapeDtypeStruct((27, chan, chan), F32),
                jax.ShapeDtypeStruct((27, chan, chan), F32),
            ),
            in_specs=[vmem] * 4,
            out_specs=(vmem, vmem, vmem),
            scratch_shapes=[
                slab,
                slab,
                slab,
                slab,
                pltpu.VMEM((4, rows, 9 * rows), BF16),
                pltpu.VMEM((depth, rows, width), F32),
                pltpu.VMEM((27 * 8, 4 * rows), F32),
                pltpu.VMEM((2, owners, tiles, 8, 128), F32),
                pltpu.VMEM((2, count - 1, tiles, 8, 128), F32),
                pltpu.VMEM((2, owners, tiles, 8, 128), F32),
                pltpu.SemaphoreType.DMA((4, 2)),
                pltpu.SemaphoreType.DMA((4, 2)),
                pltpu.SemaphoreType.DMA((2,)),
                pltpu.SemaphoreType.DMA((2,)),
                pltpu.SemaphoreType.DMA((2,)),
                pltpu.SemaphoreType.DMA((2,)),
            ],
            compiler_params=pltpu.CompilerParams(collective_id=0, has_side_effects=True),
        )(inputs[0], taps(kernel_one), taps(kernel_two), cotangent[0])
        back = lambda g: g.reshape(3, 3, 3, chan, chan).transpose(3, 4, 0, 1, 2)
        return out[None], back(g1), back(g2)

    return jax.shard_map(
        local,
        mesh=mesh,
        in_specs=(P("dp", None, "gz", None, None), P(), P(), P("dp", None, "gz", None, None)),
        out_specs=(P("dp", None, "gz", None, None), P(), P()),
        check_vma=False,
    )
```

```python
import functools
import math

import jax
import jax.numpy as jnp
from jax import lax
from jax.experimental import pallas as pl
from jax.experimental.pallas import tpu as pltpu
from jax.sharding import PartitionSpec as P

MESH = pl.DeviceIdType.MESH
F32 = jnp.float32
BF16 = jnp.bfloat16
TAPS = [(plane, col) for plane in range(3) for col in range(3)]
NN = (((1,), (0,)), ((), ()))
NT = (((1,), (1,)), ((), ()))


def dot(a, b, dims=NN):
    return lax.dot_general(a, b, dims, preferred_element_type=F32)


def iota(shape, dim):
    return lax.broadcasted_iota(jnp.int32, shape, dim)


def one_hot(mask):
    return jnp.where(mask, 1.0, 0.0).astype(BF16)


def sigmoid(v):
    return 0.5 * jnp.tanh(0.5 * v) + 0.5


def kernel(
    sizes,
    factor,
    x_hbm,
    w1_hbm,
    w2_hbm,
    cot_hbm,
    res_ref,
    sums_ref,
    x_ref,
    w1_ref,
    w2_ref,
    cot_ref,
    s_in,
    s_hid,
    s_g2,
    s_g1,
    wcat,
    slope,
    bands,
    packed,
    arrived,
    full,
    halo_send,
    halo_recv,
    rs_send,
    rs_recv,
    ag_send,
    ag_recv,
    load_sem,
):
    gz_count, dp_count, owners = sizes
    chan, depth, height, width = x_ref.shape
    rows = chan * height
    count = gz_count * dp_count
    gz = lax.axis_index("gz")
    dp = lax.axis_index("dp")
    me = gz * dp_count + dp

    def place(dev):
        return {"gz": dev // dp_count, "dp": lax.rem(dev, dp_count)}

    loads = [
        pltpu.make_async_copy(src, dst, load_sem.at[i])
        for i, (src, dst) in enumerate(
            ((w1_hbm, w1_ref), (x_hbm, x_ref), (w2_hbm, w2_ref), (cot_hbm, cot_ref))
        )
    ]
    for copy in loads:
        copy.start()

    barrier = pltpu.get_barrier_semaphore()

    def greet(k, carry):
        dev = lax.rem(me + k, count)
        pl.semaphore_signal(barrier, inc=1, device_id=place(dev), device_id_type=MESH)
        return carry

    lax.fori_loop(1, count, greet, 0)

    r, l = iota((rows, rows), 0), iota((rows, rows), 1)
    to_rows = one_hot((r // chan == l % height) & (r % chan == l // height))

    def shifts(s, p, value):
        lane = iota(value.shape, 1)
        s[0, p] = jnp.where(lane == 0, 0.0, pltpu.roll(value, 1, 1)).astype(BF16)
        s[2, p] = jnp.where(lane == width - 1, 0.0, pltpu.roll(value, width - 1, 1)).astype(BF16)

    def put(s, p, value):
        s[1, p] = value.astype(BF16)
        shifts(s, p, value)

    def up_copy(n, s):
        return pltpu.make_async_remote_copy(
            src_ref=s.at[1, depth],
            dst_ref=s.at[1, 0],
            send_sem=halo_send.at[n, 0],
            recv_sem=halo_recv.at[n, 0],
            device_id={"gz": gz + 1, "dp": dp},
            device_id_type=MESH,
        )

    def down_copy(n, s):
        return pltpu.make_async_remote_copy(
            src_ref=s.at[1, 1],
            dst_ref=s.at[1, depth + 1],
            send_sem=halo_send.at[n, 1],
            recv_sem=halo_recv.at[n, 1],
            device_id={"gz": gz - 1, "dp": dp},
            device_id_type=MESH,
        )

    def send_halo(n, s):
        @pl.when(gz < gz_count - 1)
        def _():
            up_copy(n, s).start()

        @pl.when(gz > 0)
        def _():
            down_copy(n, s).start()

    def take_halo(n, s):
        @pl.when(gz > 0)
        def _():
            up_copy(n, s).wait_recv()

        @pl.when(gz == 0)
        def _():
            s[1, 0] = jnp.zeros((rows, width), BF16)

        @pl.when(gz < gz_count - 1)
        def _():
            down_copy(n, s).wait_recv()

        @pl.when(gz == gz_count - 1)
        def _():
            s[1, depth + 1] = jnp.zeros((rows, width), BF16)

        for p in (0, depth + 1):
            shifts(s, p, s[1, p].astype(F32))

    def raw(ref, p):
        return ref[:, p].astype(F32).reshape(rows, width).astype(BF16)

    edges = sorted({0, depth - 1})
    inner = [p for p in range(depth) if p not in edges]
    groups = [edges] + [inner[i : i + 2] for i in range(0, len(inner), 2)]

    def lanes(parts):
        return parts[0] if len(parts) == 1 else jnp.concatenate(parts, axis=1)

    def load(ref, planes):
        value = dot(to_rows, lanes([raw(ref, p) for p in planes]))
        return [value[:, i * width : (i + 1) * width] for i in range(len(planes))]

    def conv(n, s, planes):
        window = jnp.concatenate(
            [lanes([s[col, p + plane] for p in planes]) for plane, col in TAPS], axis=0
        )
        value = dot(wcat[n], window)
        return [value[:, i * width : (i + 1) * width] for i in range(len(planes))]

    pack = 4 * chan
    er, el = iota((chan, pack), 0), iota((chan, pack), 1)
    eye = one_hot(iota((chan, chan), 0) == iota((chan, chan), 1))
    blank = jnp.zeros((chan, chan), BF16)
    sr, sl = iota((pack, rows), 0), iota((pack, rows), 1)

    def forward(ref):
        base = None
        for off in range(3):
            tall = jnp.concatenate([ref[9 * a + 3 * off + b] for a, b in TAPS], axis=0)
            piece = dot(tall, one_hot(el == er + off * chan))
            base = piece if base is None else base + piece
        return [base.astype(BF16)]

    def backward(ref):
        pieces = []
        for a, b in TAPS:
            tall = jnp.concatenate(
                [ref[26 - (9 * a + 3 * off + b)] for off in range(3)] + [blank], axis=0
            )
            pieces.append(dot(eye, tall, NT).astype(BF16))
        return pieces

    def spread(first, pieces):
        base = jnp.concatenate(pieces, axis=0)
        for y in range(height):
            pick = one_hot(
                (sr % chan == sl % chan)
                & (sl // chan == y - 1 + sr // chan)
                & (sr < 3 * chan)
            )
            placed = dot(base, pick).astype(BF16)
            for at in range(base.shape[0] // chan):
                n, t = first + at // 9, at % 9
                wcat[n, y * chan : (y + 1) * chan, t * rows : (t + 1) * rows] = placed[
                    at * chan : (at + 1) * chan
                ]

    def scatter_terms(j):
        def step(k, carry):
            dev = lax.rem(me + k, count)

            @pl.when(dev < owners)
            def _():
                pltpu.make_async_remote_copy(
                    src_ref=packed.at[j, dev],
                    dst_ref=arrived.at[j, count - 1 - k],
                    send_sem=rs_send.at[j],
                    recv_sem=rs_recv.at[j],
                    device_id=place(dev),
                    device_id_type=MESH,
                ).start()

            return carry

        lax.fori_loop(1, count, step, 0)

    def wait_for(ref, sem):
        pltpu.make_async_copy(ref, ref, sem).wait()

    def gather_terms(j):
        @pl.when(me < owners)
        def _():
            wait_for(arrived.at[j], rs_recv.at[j])
            full[j, me] = (jnp.sum(arrived[j], axis=0) + packed[j, me]) * factor

            def step(k, carry):
                dev = lax.rem(me + k, count)
                pltpu.make_async_remote_copy(
                    src_ref=full.at[j, me],
                    dst_ref=full.at[j, me],
                    send_sem=ag_send.at[j],
                    recv_sem=ag_recv.at[j],
                    device_id=place(dev),
                    device_id_type=MESH,
                ).start()
                return carry

            lax.fori_loop(1, count, step, 0)

    def finish_terms(j):
        @pl.when(me < owners)
        def _():
            wait_for(full.at[j, pl.ds(0, owners - 1)], ag_recv.at[j])
            wait_for(packed.at[j, pl.ds(0, owners - 1)], rs_send.at[j])
            wait_for(arrived.at[j], ag_send.at[j])

        @pl.when(me >= owners)
        def _():
            wait_for(full.at[j, pl.ds(0, owners)], ag_recv.at[j])
            wait_for(packed.at[j, pl.ds(0, owners)], rs_send.at[j])

        sums_ref[j] = full[j].reshape(owners * full.shape[2], 8, 128)[:27]

    qr, ql = iota((4 * rows, 128), 0), iota((4 * rows, 128), 1)
    gather_rows = one_hot((qr // rows == ql // chan) & (qr % chan == ql % chan))

    def terms(j, s, s_grad):
        grad = lanes([s_grad[1, p + 1] for p in range(depth)])
        block = iota((chan, rows), 1) // chan
        for plane, col in TAPS:
            window = lanes([s[col, p + plane] for p in range(depth)])
            value = dot(grad, window, NT)
            for off in range(3):
                band = jnp.zeros((chan, rows), F32)
                for y in range(height):
                    if 0 <= y + off - 1 < height:
                        part = value[y * chan : (y + 1) * chan]
                        band = jnp.where(block == y + off - 1, part, band)
                t = plane * 9 + off * 3 + col
                for g in range(4):
                    bands[t * 8 : (t + 1) * 8, g * rows : (g + 1) * rows] = band[
                        g * 8 : (g + 1) * 8
                    ]
        value = bands[...]
        high = value.astype(BF16)
        low = (value - high.astype(F32)).astype(BF16)
        total = (dot(high, gather_rows) + dot(low, gather_rows)).reshape(27, 8, 128)
        tiles = packed.shape[2]
        for t in range(27):
            packed[j, t // tiles, t % tiles] = total[t]

    if owners * packed.shape[2] > 27:
        packed[...] = jnp.zeros_like(packed)

    def first_layer(planes):
        for p, pre in zip(planes, conv(0, s_in, planes)):
            sig = sigmoid(pre)
            slope[p] = sig * (1.0 + pre * (1.0 - sig))
            put(s_hid, p + 1, pre * sig)

    def second_layer(planes):
        for p, pre, cot in zip(planes, conv(1, s_hid, planes), load(cot_ref, planes)):
            sig = sigmoid(pre)
            put(s_g2, p + 1, cot * (sig * (1.0 + pre * (1.0 - sig))))

    def second_back(planes):
        for p, value in zip(planes, conv(2, s_g2, planes)):
            put(s_g1, p + 1, value * slope[p])

    loads[0].wait()
    spread(0, forward(w1_ref))
    loads[1].wait()
    for planes in groups:
        for p, value in zip(planes, load(x_ref, planes)):
            put(s_in, p + 1, value)
    for planes in groups[1:]:
        first_layer(planes)
    pl.semaphore_wait(barrier, count - 1)
    send_halo(0, s_in)
    for copy in loads[2:]:
        copy.wait()
    spread(1, forward(w2_ref))
    take_halo(0, s_in)
    first_layer(groups[0])
    send_halo(1, s_hid)
    for planes in groups[1:]:
        second_layer(planes)
    spread(2, backward(w2_ref) + backward(w1_ref))
    take_halo(1, s_hid)
    second_layer(groups[0])
    send_halo(2, s_g2)
    terms(1, s_hid, s_g2)
    scatter_terms(1)
    take_halo(2, s_g2)
    for i, planes in enumerate(groups):
        second_back(planes)
        if i == 0:
            send_halo(3, s_g1)
    terms(0, s_in, s_g1)
    scatter_terms(0)
    gather_terms(1)
    take_halo(3, s_g1)
    for planes in groups:
        for p, value in zip(planes, conv(3, s_g1, planes)):
            res_ref[p] = value.astype(BF16)
    gather_terms(0)
    finish_terms(1)
    finish_terms(0)

    for n, s in enumerate((s_in, s_hid, s_g2, s_g1)):

        @pl.when(gz < gz_count - 1)
        def _():
            up_copy(n, s).wait_send()

        @pl.when(gz > 0)
        def _():
            down_copy(n, s).wait_send()


def unpack(res_ref, sums_ref, out_ref, g1_ref, g2_ref):
    chan, depth, height, width = out_ref.shape
    rows = chan * height
    for j, ref in enumerate((g1_ref, g2_ref)):
        for g in range(4):
            ref[:, g * 8 : (g + 1) * 8, :] = sums_ref[j, :, :, g * chan : (g + 1) * chan]
    r, l = iota((rows, rows), 0), iota((rows, rows), 1)
    to_chan = one_hot((r // height == l % chan) & (r % height == l // chan))
    for at in range(0, depth, 2):
        planes = range(at, min(at + 2, depth))
        value = dot(to_chan, jnp.concatenate([res_ref[p] for p in planes], axis=1))
        for i, p in enumerate(planes):
            part = value[:, i * width : (i + 1) * width]
            out_ref[:, p] = part.reshape(chan, height, width).astype(BF16)


def solution(mesh):
    gz_count, dp_count = mesh.shape["gz"], mesh.shape["dp"]
    count = gz_count * dp_count

    def local(inputs, kernel_one, kernel_two, cotangent):
        _, chan, depth, height, width = inputs.shape
        rows = chan * height
        cells = dp_count * gz_count * depth * height * width
        tiles = -(-27 // count)
        owners = -(-27 // tiles)
        taps = lambda k: k.transpose(2, 3, 4, 0, 1).reshape(27, chan, chan)
        slab = pltpu.VMEM((3, depth + 2, rows, width), BF16)
        vmem = pl.BlockSpec(memory_space=pltpu.VMEM)
        res, sums = pl.pallas_call(
            functools.partial(kernel, (gz_count, dp_count, owners), 1.0 / math.sqrt(cells)),
            out_shape=(
                jax.ShapeDtypeStruct((depth, rows, width), BF16),
                jax.ShapeDtypeStruct((2, 27, 8, 128), F32),
            ),
            in_specs=[pl.BlockSpec(memory_space=pl.ANY)] * 4,
            out_specs=(vmem, vmem),
            scratch_shapes=[
                pltpu.VMEM((chan, depth, height, width), BF16),
                pltpu.VMEM((27, chan, chan), BF16),
                pltpu.VMEM((27, chan, chan), BF16),
                pltpu.VMEM((chan, depth, height, width), BF16),
                slab,
                slab,
                slab,
                slab,
                pltpu.VMEM((4, rows, 9 * rows), BF16),
                pltpu.VMEM((depth, rows, width), F32),
                pltpu.VMEM((27 * 8, 4 * rows), F32),
                pltpu.VMEM((2, owners, tiles, 8, 128), F32),
                pltpu.VMEM((2, count - 1, tiles, 8, 128), F32),
                pltpu.VMEM((2, owners, tiles, 8, 128), F32),
                pltpu.SemaphoreType.DMA((4, 2)),
                pltpu.SemaphoreType.DMA((4, 2)),
                pltpu.SemaphoreType.DMA((2,)),
                pltpu.SemaphoreType.DMA((2,)),
                pltpu.SemaphoreType.DMA((2,)),
                pltpu.SemaphoreType.DMA((2,)),
                pltpu.SemaphoreType.DMA((4,)),
            ],
            compiler_params=pltpu.CompilerParams(collective_id=0, has_side_effects=True),
        )(inputs[0], taps(kernel_one), taps(kernel_two), cotangent[0])
        out, g1, g2 = pl.pallas_call(
            unpack,
            out_shape=(
                jax.ShapeDtypeStruct((chan, depth, height, width), BF16),
                jax.ShapeDtypeStruct((27, chan, chan), F32),
                jax.ShapeDtypeStruct((27, chan, chan), F32),
            ),
            in_specs=[vmem] * 2,
            out_specs=(vmem, vmem, vmem),
        )(res, sums)
        back = lambda g: g.reshape(3, 3, 3, chan, chan).transpose(3, 4, 0, 1, 2)
        return out[None], back(g1), back(g2)

    return jax.shard_map(
        local,
        mesh=mesh,
        in_specs=(P("dp", None, "gz", None, None), P(), P(), P("dp", None, "gz", None, None)),
        out_specs=(P("dp", None, "gz", None, None), P(), P()),
        check_vma=False,
    )
```
